32 devices in a mesh: seq: 2 (over core), row: 4 (over z), col: 4 (over y, x).
Axes of the slice: x: 2, y: 2, z: 4, core: 2. Of those that a mesh axis runs over, the one named last changes fastest.
Arguments:
- alignment: bfloat16 [128, 32, 256], P('seq', ('row', 'col')), may hold values from -6 to 6, as said below
- row_mask: int32 [128, 32], P('seq', ('row', 'col')), may hold values 0 or 1
- norm_gain: float32 [256], replicated, may hold values from 0.5 to 1.5
- norm_bias: float32 [256], replicated, may hold values from -1.5 to 1.5
- left_weight: bfloat16 [256, 32], replicated, may hold values from -0.375 to 0.375
- left_bias: float32 [32], replicated, may hold values from -6 to 6
- right_weight: bfloat16 [256, 32], replicated, may hold values from -0.375 to 0.375
- right_bias: float32 [32], replicated, may hold values from -6 to 6
- pair_weight: float32 [1024, 128], replicated, may hold values from -0.375 to 0.375
- pair_state: bfloat16 [32, 32, 128], P('row', 'col'), may hold values from -6 to 6
Outputs:
- new_pair: bfloat16 [32, 32, 128], P('row', 'col')
The draws below stay inside these ranges and needn't reach their ends.
Inputs may be any that keep to these rules, and one draw needn't show every extreme that they name: alignment rows come in 8 clusters of consecutive rows that share a profile per residue, entries within -6 to 6.
All inputs are finite; a program needn't handle non-finite values.
Results may differ from the reference program's by a relative error of at most 0.001.
Values may be sent and summed in bfloat16 or wider, within the bound.
A program may use at most 64 MiB of HBM per device.

```python
import jax
import jax.numpy as jnp
from jax import lax

CM = 256
CH = 32
CZ = 128
CLUST = 8
S = 128
R = 32


def draw_alignment(key, part):
    first_key, second_key = jax.random.split(jax.random.fold_in(key, 11))
    group = jnp.arange(S) * CLUST // S
    centers = jax.random.normal(first_key, (CLUST, R, CM), jnp.float32)
    noise = 0.5 * jax.random.normal(second_key, (S, R, CM), jnp.float32)
    values = jnp.clip(centers[group] + noise, -6.0, 6.0)
    return values.astype(jnp.bfloat16)


def with_ends(array, rng, smallest, largest):
    longest = array.shape.index(max(array.shape))
    spots = []
    for shift in (0, 1):
        where = [jax.random.randint(jax.random.fold_in(rng, axis), (), 0, length) for axis, length in enumerate(array.shape)]
        where[longest] = (where[longest] + shift) % array.shape[longest]
        spots.append(tuple(where))
    return array.at[spots[0]].set(smallest).at[spots[1]].set(largest)


def levels(stream_key, extent, cuts, least, top_value):
    gain, own = 1.0, jax.random.fold_in(stream_key, 6)
    for dim, parts in cuts:
        steps = jnp.exp(jax.random.uniform(jax.random.fold_in(own, dim), (parts,), jnp.float32, least / len(cuts), top_value / len(cuts)))
        gain = gain * jnp.repeat(steps, extent[dim] // parts).reshape([-1 if axis == dim else 1 for axis in range(len(extent))])
    return gain


def bell_draw(own_key, shape, deviation, most, cuts=(), held_as=jnp.bfloat16):
    loudness = levels(own_key, shape, cuts, -0.22, 0.18) if cuts else 1.0
    drawn = jax.random.normal(own_key, shape, jnp.float32) * deviation * loudness
    return jnp.minimum(jnp.maximum(drawn, -most), most).astype(held_as)


def setup_inputs(seed: int = 0) -> dict:
    key_list = jax.random.split(jax.random.key(seed), 11)
    alignment = draw_alignment(jax.random.fold_in(key_list[10], 71), 0)
    row_mask = with_ends((jax.random.randint(key_list[1], (S, R), 0, 8) < 7).astype(jnp.int32), jax.random.fold_in(key_list[1], 1), 0, 1)
    norm_gain = jnp.clip(1.0 + 0.1 * jax.random.normal(key_list[2], (CM,), jnp.float32), 0.5, 1.5)
    norm_bias = bell_draw(key_list[3], (CM,), 0.1, 1.5, (), jnp.float32)
    left_weight = bell_draw(key_list[4], (CM, CH), CM ** -0.5, 0.375)
    left_bias = bell_draw(key_list[5], (CH,), 0.5, 6.0, (), jnp.float32)
    right_weight = bell_draw(key_list[6], (CM, CH), CM ** -0.5, 0.375)
    right_bias = bell_draw(key_list[7], (CH,), 0.5, 6.0, (), jnp.float32)
    pair_weight = bell_draw(key_list[8], (CH * CH, CZ), (CH * CH // 4) ** -0.5, 0.375, (), jnp.float32)
    pair_state = bell_draw(key_list[9], (R, R, CZ), 0.5, 6.0, ((0, 4), (1, 4)))
    return {"alignment": alignment, "row_mask": row_mask, "norm_gain": norm_gain, "norm_bias": norm_bias, "left_weight": left_weight, "left_bias": left_bias, "right_weight": right_weight, "right_bias": right_bias, "pair_weight": pair_weight, "pair_state": pair_state}


variance_floor = 1e-05
count_floor = 0.001

def layer_norm(alignment, norm_gain, norm_bias):
    values = alignment.astype(jnp.float32)
    center = lax.optimization_barrier(jnp.mean(values, axis=-1, keepdims=True))
    spread = lax.optimization_barrier(jnp.mean((values - center) ** 2, axis=-1, keepdims=True))
    return ((values - center) * lax.rsqrt(spread + variance_floor) * norm_gain + norm_bias).astype(jnp.bfloat16)

def reference(alignment, row_mask, norm_gain, norm_bias, left_weight, left_bias, right_weight, right_bias, pair_weight, pair_state):
    normed = layer_norm(alignment, norm_gain, norm_bias)
    mask_float = row_mask.astype(jnp.float32)
    left = ((jnp.dot(normed, left_weight, preferred_element_type=jnp.float32) + left_bias) * mask_float[:, :, None]).astype(jnp.bfloat16)
    right = ((jnp.dot(normed, right_weight, preferred_element_type=jnp.float32) + right_bias) * mask_float[:, :, None]).astype(jnp.bfloat16)
    outer = jnp.einsum('sic,sje->ijce', left.astype(jnp.float32), right.astype(jnp.float32))
    outer = outer.reshape(outer.shape[0], outer.shape[1], outer.shape[2] * outer.shape[3])
    counts = jnp.dot(mask_float.T, mask_float, precision=lax.Precision.HIGHEST)
    update = jnp.dot(outer, pair_weight, precision=lax.Precision.HIGHEST) / (count_floor + counts)[:, :, None]
    return (pair_state.astype(jnp.float32) + update).astype(jnp.bfloat16)
```

```python
import functools

import jax
import jax.numpy as jnp
from jax import lax
from jax.experimental import pallas as pl
from jax.experimental.pallas import tpu as pltpu
from jax.sharding import PartitionSpec as P

variance_floor = 1e-05
count_floor = 0.001
LANES = 128
MESH = pl.DeviceIdType.MESH
NT = (((1,), (1,)), ((), ()))


def device(seq, row, col):
    return {"seq": seq, "row": row, "col": col}


def kernel(
    sizes,
    x_hbm, mask_hbm, gain_hbm, shift_hbm, wl_hbm, bl_hbm, wr_hbm, br_hbm, pw_hbm, pair_hbm,
    out_ref,
    x_v, xf_v, mask_v, gain_v, shift_v, w_v, bl_v, br_v, pw_v, pair_v, w2_v,
    lbuf, rbuf, rsend, mlbuf, mrbuf, msend, cbuf, pbuf, prod_v, flat_v,
    in_sem,
    l_send, l_recv, r_send, r_recv, ml_send, ml_recv, mr_send, mr_recv,
    c_send, c_recv, p_send, p_recv,
):
    nseq, nrow, ncol, S, nres, CM, CH = sizes
    nI, nJ = ncol * nres, nrow * nres
    G = LANES // CH
    s, r, c = lax.axis_index("seq"), lax.axis_index("row"), lax.axis_index("col")
    q = r * ncol + c
    target_col, slot = q // nrow, q % nrow
    is_self = target_col == c

    def right_source(t):
        owner = c * nrow + t
        return owner, device(s, owner // ncol, owner % ncol)

    barrier = pltpu.get_barrier_semaphore()
    for d in range(1, ncol):
        pl.semaphore_signal(
            barrier, inc=1, device_id=device(s, r, (c + ncol - d) % ncol), device_id_type=MESH
        )
    for t in range(nrow):
        owner, where = right_source(t)

        @pl.when(owner != q)
        def _():
            pl.semaphore_signal(barrier, inc=1, device_id=where, device_id_type=MESH)

    for d in range(1, nseq):
        pl.semaphore_signal(
            barrier, inc=1, device_id=device((s + nseq - d) % nseq, r, c), device_id_type=MESH
        )

    pairs = [
        (mask_hbm, mask_v),
        (x_hbm, x_v),
        (gain_hbm, gain_v),
        (shift_hbm, shift_v),
        (wl_hbm, w_v.at[pl.ds(0, CH)]),
        (wr_hbm, w_v.at[pl.ds(CH, CH)]),
        (bl_hbm, bl_v),
        (br_hbm, br_v),
        (pw_hbm, pw_v),
        (pair_hbm, pair_v),
    ]
    local = [pltpu.make_async_copy(a, b, in_sem.at[k]) for k, (a, b) in enumerate(pairs)]
    for copy in local:
        copy.start()

    def left_copy(d, src, dst, send, recv):
        return pltpu.make_async_remote_copy(
            src_ref=src, dst_ref=dst.at[c], send_sem=send.at[d], recv_sem=recv.at[c],
            device_id=device(s, r, (c + d) % ncol), device_id_type=MESH,
        )

    def right_copy(d, src, dst, send, recv):
        return pltpu.make_async_remote_copy(
            src_ref=src, dst_ref=dst.at[slot], send_sem=send.at[d], recv_sem=recv.at[slot],
            device_id=device(s, (r + d) % nrow, target_col), device_id_type=MESH,
        )

    def seq_copy(d, buf, send, recv):
        return pltpu.make_async_remote_copy(
            src_ref=buf.at[s], dst_ref=buf.at[s], send_sem=send.at[d], recv_sem=recv.at[s],
            device_id=device((s + d) % nseq, r, c), device_id_type=MESH,
        )

    def start_left(src, dst, send, recv):
        for d in reversed(range(1, ncol)):
            left_copy(d, src, dst, send, recv).start()

    def start_right(src, dst, send, recv):
        for d in reversed(range(1, nrow)):
            right_copy(d, src, dst, send, recv).start()

        @pl.when(jnp.logical_not(is_self))
        def _():
            right_copy(0, src, dst, send, recv).start()

    def arrive_left(dst, send, recv):
        for d in range(1, ncol):
            peer = (c + d) % ncol
            pltpu.make_async_remote_copy(
                src_ref=dst.at[peer], dst_ref=dst.at[peer], send_sem=send.at[d],
                recv_sem=recv.at[peer], device_id=device(s, r, peer), device_id_type=MESH,
            ).wait_recv()

    def arrive_right(dst, send, recv):
        for t in range(nrow):
            owner, where = right_source(t)

            @pl.when(owner != q)
            def _():
                pltpu.make_async_remote_copy(
                    src_ref=dst.at[t], dst_ref=dst.at[t], send_sem=send.at[0],
                    recv_sem=recv.at[t], device_id=where, device_id_type=MESH,
                ).wait_recv()

    def arrive_seq(buf, send, recv):
        for d in range(1, nseq):
            peer = (s + d) % nseq
            pltpu.make_async_remote_copy(
                src_ref=buf.at[peer], dst_ref=buf.at[peer], send_sem=send.at[d],
                recv_sem=recv.at[peer], device_id=device(peer, r, c), device_id_type=MESH,
            ).wait_recv()

    local[0].wait()
    mask_row = jnp.concatenate(
        [mask_v[k : k + 1, :].astype(jnp.float32) for k in range(nres)], axis=1
    )
    mask_block = jnp.broadcast_to(mask_row, (8, nres * S))
    mlbuf[c] = mask_block
    msend[...] = mask_block

    @pl.when(is_self)
    def _():
        mrbuf[slot] = mask_block

    pl.semaphore_wait(barrier, ncol - 1 + nseq - 1 + nrow - is_self.astype(jnp.int32))
    start_left(msend, mlbuf, ml_send, ml_recv)
    start_right(msend, mrbuf, mr_send, mr_recv)

    for copy in local[1:8]:
        copy.wait()
    H = CM // LANES
    xf_v[...] = x_v[...].astype(jnp.float32)
    halves = [
        jnp.concatenate(
            [xf_v[pl.ds(h * nres + k, S, stride=H * nres), :] for k in range(nres)], axis=0
        )
        for h in range(H)
    ]
    center = sum(jnp.sum(v, axis=-1, keepdims=True) for v in halves) * (1.0 / CM)
    halves = [v - center for v in halves]
    spread = sum(jnp.sum(v * v, axis=-1, keepdims=True) for v in halves) * (1.0 / CM)
    scale = lax.rsqrt(spread + variance_floor)
    normed = jnp.concatenate(
        [
            (
                v * scale * gain_v[:, h * LANES : (h + 1) * LANES]
                + shift_v[:, h * LANES : (h + 1) * LANES]
            ).astype(jnp.bfloat16)
            for h, v in enumerate(halves)
        ],
        axis=1,
    )
    offsets = jnp.concatenate(
        [bl_v[...], br_v[...], jnp.zeros((1, LANES - 2 * CH), jnp.float32)], axis=1
    )
    offset_column = jnp.broadcast_to(offsets, (LANES, LANES)).T[: 2 * CH, :]
    both = lax.dot_general(w_v[...], normed, NT, preferred_element_type=jnp.float32)
    both = ((both + offset_column) * mask_row).astype(jnp.bfloat16)
    rsend[...] = both[CH:, :]
    lbuf[c] = both[:CH, :]

    @pl.when(is_self)
    def _():
        rbuf[slot] = both[CH:, :]

    start_right(rsend, rbuf, r_send, r_recv)
    start_left(lbuf.at[c], lbuf, l_send, l_recv)

    local[8].wait()
    local[9].wait()
    weight = pw_v[...]
    high = weight.astype(jnp.bfloat16)
    w2_v[:, :LANES] = high
    w2_v[:, LANES:] = (weight - high.astype(jnp.float32)).astype(jnp.bfloat16)

    def stack(buf, count, rows):
        return jnp.concatenate(
            [buf[d, :rows, k * S : (k + 1) * S] for d in range(count) for k in range(nres)], axis=0
        )

    arrive_left(mlbuf, ml_send, ml_recv)
    arrive_right(mrbuf, mr_send, mr_recv)
    row_masks = jnp.concatenate(
        [stack(mlbuf, ncol, 1), jnp.zeros((LANES - nI, S), jnp.float32)], axis=0
    )
    cbuf[s] = lax.dot_general(
        stack(mrbuf, nrow, 1).astype(jnp.bfloat16),
        row_masks.astype(jnp.bfloat16),
        NT,
        preferred_element_type=jnp.float32,
    )
    for d in range(1, nseq):
        seq_copy(d, cbuf, c_send, c_recv).start()

    arrive_left(lbuf, l_send, l_recv)
    arrive_right(rbuf, r_send, r_recv)
    product = lax.dot_general(
        stack(lbuf, ncol, CH), stack(rbuf, nrow, CH), NT, preferred_element_type=jnp.float32
    )
    for t in range(nJ // G):
        prod_v[t] = product[:, t * LANES : (t + 1) * LANES]
    for group in range(nI // 8):
        for g in range(CH // G):
            for t in range(nJ // G):
                rows = [
                    prod_v[t, pl.ds(group * 8 * CH + g * G + k, 8, stride=CH), :] for k in range(G)
                ]
                for j in range(G):
                    base = (group * nJ + t * G + j) * 8
                    flat_v[base : base + 8, g * LANES : (g + 1) * LANES] = jnp.concatenate(
                        [v[:, j * CH : (j + 1) * CH] for v in rows], axis=1
                    )
    flat = flat_v[...]
    flat_high = flat.astype(jnp.bfloat16)
    flat_low = (flat - flat_high.astype(jnp.float32)).astype(jnp.bfloat16)
    wide = jnp.dot(flat_high, w2_v[...], preferred_element_type=jnp.float32)
    narrow = jnp.dot(flat_low, w2_v[:, :LANES], preferred_element_type=jnp.float32)
    pbuf[s] = wide[:, :LANES] + (wide[:, LANES:] + narrow)
    for d in range(1, nseq):
        seq_copy(d, pbuf, p_send, p_recv).start()

    arrive_seq(cbuf, c_send, c_recv)
    inverse = 1.0 / (count_floor + sum(cbuf[k] for k in range(nseq)))
    arrive_seq(pbuf, p_send, p_recv)
    for i in range(nI):
        start = (i // 8) * nJ * 8 + i % 8
        total = sum(pbuf[k, pl.ds(start, nJ, stride=8), :] for k in range(nseq))
        out_ref[i] = (
            pair_v[i].astype(jnp.float32) + total * inverse[:, i : i + 1]
        ).astype(jnp.bfloat16)

    for d in range(1, ncol):
        left_copy(d, msend, mlbuf, ml_send, ml_recv).wait_send()
        left_copy(d, lbuf.at[c], lbuf, l_send, l_recv).wait_send()
    for d in range(1, nrow):
        right_copy(d, msend, mrbuf, mr_send, mr_recv).wait_send()
        right_copy(d, rsend, rbuf, r_send, r_recv).wait_send()

    @pl.when(jnp.logical_not(is_self))
    def _():
        right_copy(0, msend, mrbuf, mr_send, mr_recv).wait_send()
        right_copy(0, rsend, rbuf, r_send, r_recv).wait_send()

    for d in range(1, nseq):
        seq_copy(d, cbuf, c_send, c_recv).wait_send()
        seq_copy(d, pbuf, p_send, p_recv).wait_send()


def on_device(
    nseq, nrow, ncol,
    alignment, row_mask, norm_gain, norm_bias, left_weight, left_bias,
    right_weight, right_bias, pair_weight, pair_state,
):
    S, nres, CM = alignment.shape
    CH = left_weight.shape[1]
    CZ = pair_weight.shape[1]
    H = CM // LANES
    nI, nJ = ncol * nres, nrow * nres
    f32, bf16 = jnp.float32, jnp.bfloat16
    view = (
        alignment.reshape(S, nres, H, LANES).transpose(0, 2, 1, 3).reshape(S * H * nres, LANES)
    )
    dma = pltpu.SemaphoreType.DMA
    return pl.pallas_call(
        functools.partial(kernel, (nseq, nrow, ncol, S, nres, CM, CH)),
        out_shape=jax.ShapeDtypeStruct(pair_state.shape, bf16),
        in_specs=[pl.BlockSpec(memory_space=pl.ANY)] * 10,
        out_specs=pl.BlockSpec(memory_space=pltpu.VMEM),
        scratch_shapes=[
            pltpu.VMEM((S * H * nres, LANES), bf16),
            pltpu.VMEM((S * H * nres, LANES), f32),
            pltpu.VMEM((nres, S), jnp.int32),
            pltpu.VMEM((1, CM), f32),
            pltpu.VMEM((1, CM), f32),
            pltpu.VMEM((2 * CH, CM), bf16),
            pltpu.VMEM((1, CH), f32),
            pltpu.VMEM((1, CH), f32),
            pltpu.VMEM(pair_weight.shape, f32),
            pltpu.VMEM(pair_state.shape, bf16),
            pltpu.VMEM((CH * CH, 2 * CZ), bf16),
            pltpu.VMEM((ncol, CH, nres * S), bf16),
            pltpu.VMEM((nrow, CH, nres * S), bf16),
            pltpu.VMEM((CH, nres * S), bf16),
            pltpu.VMEM((ncol, 8, nres * S), f32),
            pltpu.VMEM((nrow, 8, nres * S), f32),
            pltpu.VMEM((8, nres * S), f32),
            pltpu.VMEM((nseq, nJ, LANES), f32),
            pltpu.VMEM((nseq, nI * nJ, CZ), f32),
            pltpu.VMEM((nJ * CH // LANES, nI * CH, LANES), f32),
            pltpu.VMEM((nI * nJ, CH * CH), f32),
            dma((10,)),
            dma((ncol,)), dma((ncol,)), dma((nrow,)), dma((nrow,)),
            dma((ncol,)), dma((ncol,)), dma((nrow,)), dma((nrow,)),
            dma((nseq,)), dma((nseq,)), dma((nseq,)), dma((nseq,)),
        ],
        compiler_params=pltpu.CompilerParams(collective_id=0, has_side_effects=True),
    )(
        view,
        row_mask.T,
        norm_gain.reshape(1, CM),
        norm_bias.reshape(1, CM),
        left_weight.T,
        left_bias.reshape(1, CH),
        right_weight.T,
        right_bias.reshape(1, CH),
        pair_weight,
        pair_state,
    )


def solution(mesh):
    placed = (
        P("seq", ("row", "col"), None),
        P("seq", ("row", "col")),
        P(), P(), P(), P(), P(), P(), P(),
        P("row", "col", None),
    )
    return jax.shard_map(
        functools.partial(
            on_device, mesh.shape["seq"], mesh.shape["row"], mesh.shape["col"]
        ),
        mesh=mesh, in_specs=placed, out_specs=P("row", "col", None), check_vma=False,
    )
```
